512 devices in a mesh: dp: 64 (over z_lo, x, core), ens: 8 (over y, z_hi).
Axes of the slice: x: 4, y: 4, z: 16 (z_hi: 2, z_lo: 8; z = z_hi * 8 + z_lo), core: 2. Of those that a mesh axis runs over, the one named last changes fastest.
Arguments:
- embeddings: bfloat16 [49152, 1024], P('dp'), may hold values from -6 to 6
- valid_mask: int32 [49152], P('dp'), may hold values 0 or 1
- first_weight: bfloat16 [8, 1024, 4096], P(None, 'dp', 'ens'), may hold values from -0.1875 to 0.1875
- second_weight: bfloat16 [8, 4096, 128], P(None, 'ens'), may hold values from -0.09375 to 0.09375
- thresholds: int32 [8], replicated, may hold values from -256 to 256
Outputs:
- mean_logits: float32 [49152, 128], P('dp')
- kept_share: float32 [8], P('ens')
- agree_share: float32 [8], P('ens')
The draws below stay inside these ranges and needn't reach their ends.
All inputs are finite; a program needn't handle non-finite values. No bound on the sum of `valid_mask` on one device may be relied on, other than what follows from the above.
Results may differ from the reference program's by a relative error of at most 0.0044.
Values may be sent and summed in bfloat16 or wider, within the bound.
A program may use at most 64 MiB of HBM per device.

```python
import jax
import jax.numpy as jnp
from jax import lax

D = 1024
H = 4096
C = 128
DOC_DEV = 768
MEMBERS = 8
DOCS = 49152
N_DP = 64


def with_ends(array, stream_key, low, largest):
    index_at = [jax.random.randint(jax.random.fold_in(stream_key, axis), (), 0, length) for axis, length in enumerate(array.shape)]
    widest = array.shape.index(max(array.shape))
    next_to = index_at[:widest] + [(index_at[widest] + 1) % array.shape[widest]] + index_at[widest + 1:]
    return array.at[tuple(index_at)].set(low).at[tuple(next_to)].set(largest)


def block_scale(own_key, extent, split, least, high):
    loudness = 1.0
    for position, blocks in split:
        heights = jax.random.uniform(jax.random.fold_in(jax.random.fold_in(own_key, 6), position), (blocks,), jnp.float32, least / len(split), high / len(split))
        loudness = loudness * jnp.repeat(jnp.exp(heights), extent[position] // blocks).reshape((-1,) + (1,) * (len(extent) - 1 - position))
    return loudness


def noise(own_key, dims, scale, reach, pieces=(), kind=jnp.bfloat16):
    entries = jax.random.normal(own_key, dims, jnp.float32) * scale
    if len(pieces) > 0:
        entries = block_scale(own_key, dims, pieces, -0.22, 0.18) * entries
    return jnp.clip(entries, min=-reach, max=reach).astype(kind)


def setup_inputs(seed: int = 0) -> dict:
    seeds = jax.random.split(jax.random.key(seed), 6)
    return {
        "embeddings": noise(seeds[0], (DOCS, D), 1.0, 6.0, ((0, 64),)),
        "valid_mask": with_ends((jax.random.randint(seeds[1], (DOCS,), 0, 4) < 3).astype(jnp.int32), jax.random.fold_in(seeds[1], 1), 0, 1),
        "first_weight": noise(seeds[2], (MEMBERS, D, H), D ** -0.5, 0.1875, ((1, 64), (2, 8))),
        "second_weight": noise(seeds[3], (MEMBERS, H, C), H ** -0.5, 0.09375, ((1, 8),)),
        "thresholds": with_ends(jax.random.randint(seeds[4], (MEMBERS,), -256, 257), jax.random.fold_in(seeds[4], 1), -256, 256).astype(jnp.int32),
    }


def member_logits(embeddings, first_weight, second_weight):
    blocks = embeddings.reshape(N_DP, DOC_DEV, D)

    def one_member(weights):
        layer_one, layer_two = weights

        def one_block(block_rows):
            hidden = jnp.maximum(jnp.dot(block_rows, layer_one, preferred_element_type=jnp.float32), 0.0).astype(jnp.bfloat16)
            return jnp.dot(hidden, layer_two, preferred_element_type=jnp.float32)
        return lax.map(one_block, blocks).reshape(DOCS, C)
    return lax.map(one_member, (first_weight, second_weight))

def reference(embeddings, valid_mask, first_weight, second_weight, thresholds):
    logits = member_logits(embeddings, first_weight, second_weight)
    mean_logits = lax.optimization_barrier(jnp.sum(logits, axis=0)) / MEMBERS
    levels = jnp.arange(C, dtype=jnp.float32)
    grades = (2.0 * levels / (C - 1) - 1.0) * jnp.sqrt(jnp.float32(3.0 / C))
    scores = jnp.einsum('edc,c->ed', logits, grades, precision=lax.Precision.HIGHEST)
    ens_score = jnp.dot(mean_logits, grades, precision=lax.Precision.HIGHEST)
    cutoffs = thresholds.astype(jnp.float32) / 256.0
    validity = valid_mask.astype(jnp.float32)
    kept_soft = validity[None, :] * jax.nn.sigmoid(4.0 * (scores - cutoffs[:, None]))
    ens_kept = jax.nn.sigmoid(4.0 * (ens_score - jnp.mean(cutoffs)))
    kept_share = lax.optimization_barrier(jnp.sum(kept_soft, axis=1)) / DOC_DEV
    agree_share = lax.optimization_barrier(jnp.sum(kept_soft * ens_kept[None, :], axis=1)) / DOC_DEV
    return (mean_logits, kept_share, agree_share)
```

```python
import functools

import jax
import jax.numpy as jnp
from jax import lax
from jax.experimental import pallas as pl
from jax.experimental.pallas import tpu as pltpu
from jax.sharding import PartitionSpec as P

MESH = pl.DeviceIdType.MESH
NZ, NX, NC, NY, NH = 8, 4, 2, 4, 2
CHUNKS = 4
DELTA = 2


def kernel(
    emb_hbm, mask_ref, fw_hbm, sw_hbm, thr_ref, out_ref, kept_ref, agree_ref,
    w, emb, bmat, acc, part_s, part_r, sc_s, sc_r, zp_s, zp_r, zc_s, zc_r, fin, mask4, tot1, tot2,
    in_sem, z_recv, x_recv, d_recv, z_send, x_send, d_send, y_send, y_recv, h_send, h_recv, t_send, t_recv,
):
    members, _, rows, units = fw_hbm.shape[0], 0, fw_hbm.shape[1], fw_hbm.shape[2]
    docs, classes = out_ref.shape
    share = docs // NY
    per = members // CHUNKS
    me = lax.axis_index("dp")
    ens = lax.axis_index("ens")
    core = lax.rem(me, NC)
    x = lax.rem(me // NC, NX)
    z = me // (NC * NX)
    y = ens // NH
    zh = lax.rem(ens, NH)

    def dp_of(z_, x_, c_):
        return (z_ * NX + x_) * NC + c_

    x_up, x_dn, x_far = lax.rem(x + 1, NX), lax.rem(x + NX - 1, NX), lax.rem(x + 2, NX)
    sib = {"dp": dp_of(z, x, 1 - core)}
    to_xu = {"dp": dp_of(z, x_up, core)}
    to_xd = {"dp": dp_of(z, x_dn, core)}
    to_zu = {"dp": dp_of(z + 1, x, core)}
    to_zd = {"dp": dp_of(z - 1, x, core)}
    has_zu, has_zd = z + 1 < NZ, z > 0

    own_in = pltpu.make_async_copy(fw_hbm, w.at[:, z, x * NC + core], in_sem.at[0])
    emb_in = pltpu.make_async_copy(emb_hbm, emb, in_sem.at[1])
    sw_in = pltpu.make_async_copy(sw_hbm, bmat.at[:, :, pl.ds(0, classes)], in_sem.at[2])
    own_in.start()
    sw_in.start()
    emb_in.start()

    barrier = pltpu.get_barrier_semaphore()
    for d in (to_xu, to_xd, sib):
        pl.semaphore_signal(barrier, inc=1, device_id=d, device_id_type=MESH)
    for k in range(1, NY * NH):
        pl.semaphore_signal(
            barrier, inc=1, device_id={"ens": lax.rem(ens + k, NY * NH)}, device_id_type=MESH
        )
    for ok, d in ((has_zu, to_zu), (has_zd, to_zd)):
        @pl.when(ok)
        def _():
            pl.semaphore_signal(barrier, inc=1, device_id=d, device_id_type=MESH)
    pl.semaphore_wait(
        barrier, jnp.int32(3 + NY * NH - 1) + has_zu.astype(jnp.int32) + has_zd.astype(jnp.int32)
    )

    acc[...] = jnp.zeros_like(acc)

    def piece(h, zo, xo):
        return w.at[pl.ds(h * per, per), zo, xo * NC + core]

    def rcopy(ref, send, recv, to):
        return pltpu.make_async_remote_copy(
            src_ref=ref, dst_ref=ref, send_sem=send, recv_sem=recv, device_id=to, device_id_type=MESH
        )

    def to_sibling(h, zo, xo):
        rcopy(piece(h, zo, xo), d_send.at[0], d_recv.at[h], sib).start()

    def x_out(h, zo):
        rcopy(piece(h, zo, x), x_send.at[0], x_recv.at[h, zo, 0], to_xu).start()
        rcopy(piece(h, zo, x), x_send.at[1], x_recv.at[h, zo, 1], to_xd).start()
        to_sibling(h, zo, x)

    def z_out(h, zo, s, up):
        if up:
            rcopy(piece(h, zo, x), z_send.at[0, s], z_recv.at[h, zo], to_zu).start()
        else:
            rcopy(piece(h, zo, x), z_send.at[1, s], z_recv.at[h, zo], to_zd).start()

    def plus_way(h, zo):
        flip = (zo > z).astype(jnp.int32)
        return lax.rem(zo + flip + h, 2) == 0

    def z_event(h, s):
        @pl.when(s == 0)
        def _():
            @pl.when(has_zu)
            def _():
                z_out(h, z, s, True)

            @pl.when(has_zd)
            def _():
                z_out(h, z, s, False)
            x_out(h, z)

        for up in (True, False):
            zo = z - s if up else z + s

            @pl.when((s > 0) & (zo >= 0) & (zo < NZ))
            def _():
                rcopy(piece(h, zo, x), z_send.at[0, 0], z_recv.at[h, zo], to_xu).wait_recv()

                @pl.when(has_zu if up else has_zd)
                def _():
                    z_out(h, zo, s, up)
                x_out(h, zo)

    def both_ways(s, act):
        @pl.when((s >= 0) & (s < NZ) & (z - s >= 0))
        def _():
            act(z - s)

        @pl.when((s > 0) & (s < NZ) & (z + s < NZ))
        def _():
            act(z + s)

    def x_event(h, s):
        def act(zo):
            plus = plus_way(h, zo)
            rcopy(piece(h, zo, x_dn), x_send.at[2], x_recv.at[h, zo, 0], to_xu).wait_recv()

            @pl.when(plus)
            def _():
                rcopy(piece(h, zo, x_dn), x_send.at[2], x_recv.at[h, zo, 2], to_xu).start()
            to_sibling(h, zo, x_dn)
            rcopy(piece(h, zo, x_up), x_send.at[2], x_recv.at[h, zo, 1], to_xu).wait_recv()

            @pl.when(jnp.logical_not(plus))
            def _():
                rcopy(piece(h, zo, x_up), x_send.at[2], x_recv.at[h, zo, 2], to_xd).start()
            to_sibling(h, zo, x_up)
        both_ways(s, act)

    def far_event(h, s):
        def act(zo):
            rcopy(piece(h, zo, x_far), x_send.at[2], x_recv.at[h, zo, 2], to_xu).wait_recv()
            to_sibling(h, zo, x_far)
        both_ways(s, act)

    level = lax.broadcasted_iota(jnp.int32, (units, classes), 1)
    grade = (2.0 * level.astype(jnp.float32) / (classes - 1) - 1.0) * jnp.sqrt(jnp.float32(3.0 / classes))

    def grade_column(m):
        column = jnp.sum(bmat[m, :, 0:classes].astype(jnp.float32) * grade, axis=1, keepdims=True)
        high = column.astype(jnp.bfloat16).astype(jnp.float32)
        mid = (column - high).astype(jnp.bfloat16).astype(jnp.float32)
        low = column - high - mid
        both = jnp.where(level == m, high, jnp.where(level == members + m, mid, jnp.where(level == 2 * members + m, low, 0.0)))
        bmat[m, :, classes:2 * classes] = both.astype(jnp.bfloat16)

    def compute(m):
        if CHUNKS == members:
            arrived = True
        else:
            arrived = lax.rem(m, per) == 0

        @pl.when(arrived)
        def _():
            h = m // per
            size = w.at[pl.ds(0, per), :, pl.ds(0, NX)]
            rcopy(size, d_send.at[0], d_recv.at[h], sib).wait_recv()
        hidden = jnp.maximum(
            jnp.dot(emb[...], w[m].reshape(NZ * NX * NC * rows, units), preferred_element_type=jnp.float32), 0.0
        ).astype(jnp.bfloat16)
        acc[...] += jnp.dot(hidden, bmat[m], preferred_element_type=jnp.float32)

    lag = NZ + 2

    def slot(t, carry):
        @pl.when(t == 0)
        def _():
            own_in.wait()
        for h in range(CHUNKS):
            s = t - DELTA * h

            @pl.when((s >= 0) & (s < NZ))
            def _():
                z_event(h, s)
        for h in range(CHUNKS):
            x_event(h, t - DELTA * h - 1)
        for h in range(CHUNKS):
            far_event(h, t - DELTA * h - 2)

        @pl.when(t == 0)
        def _():
            sw_in.wait()
            emb_in.wait()

        @pl.when(t < members)
        def _():
            grade_column(t)

        @pl.when(t >= lag)
        def _():
            compute(t - lag)
        return carry

    lax.fori_loop(0, lag + members, slot, 0)

    for j in range(NY):
        rows_j = jnp.concatenate(
            [acc[j * share:(j + 1) * share, classes:2 * classes], jnp.zeros((256 - share, classes), jnp.float32)], axis=0
        )
        turned = rows_j.T
        sc_s[j] = turned[0:8] + turned[8:16] + turned[16:24]

    def y_dev(k):
        return {"ens": lax.rem(y + k, NY) * NH + zh}

    def sc_copy(k):
        return pltpu.make_async_remote_copy(
            src_ref=sc_s.at[lax.rem(y + k, NY)], dst_ref=sc_r.at[y], send_sem=y_send.at[0, k], recv_sem=y_recv.at[0, y],
            device_id=y_dev(k), device_id_type=MESH,
        )

    def part_copy(k):
        return pltpu.make_async_remote_copy(
            src_ref=part_s.at[lax.rem(y + k, NY)], dst_ref=part_r.at[y], send_sem=y_send.at[1, k], recv_sem=y_recv.at[1, y],
            device_id=y_dev(k), device_id_type=MESH,
        )

    def fin_copy(k):
        return pltpu.make_async_remote_copy(
            src_ref=fin.at[y], dst_ref=fin.at[y], send_sem=y_send.at[2, k], recv_sem=y_recv.at[2, y],
            device_id=y_dev(k), device_id_type=MESH,
        )

    def y_wait(i, buf, k):
        other = lax.rem(y + k, NY)
        rcopy(buf.at[other], y_send.at[i, k], y_recv.at[i, other], y_dev(k)).wait_recv()

    for k in range(1, NY):
        sc_copy(k).start()
    for j in range(NY):
        part_s[j] = (acc[j * share:(j + 1) * share, 0:classes] * (1.0 / members)).astype(jnp.bfloat16)
    for k in range(1, NY):
        part_copy(k).start()

    z_dev = {"ens": y * NH + (1 - zh)}
    zc_copy = pltpu.make_async_remote_copy(
        src_ref=zc_s, dst_ref=zc_r, send_sem=h_send.at[0], recv_sem=h_recv.at[0], device_id=z_dev, device_id_type=MESH
    )
    zp_copy = pltpu.make_async_remote_copy(
        src_ref=zp_s, dst_ref=zp_r, send_sem=h_send.at[1], recv_sem=h_recv.at[1], device_id=z_dev, device_id_type=MESH
    )
    scores = sc_s[y]
    for k in range(1, NY):
        y_wait(0, sc_r, k)
        scores += sc_r[lax.rem(y + k, NY)]
    zc_s[...] = scores
    zc_copy.start()
    means = acc[pl.ds(pl.multiple_of(y * share, share), share), 0:classes] * (1.0 / members)
    for k in range(1, NY):
        y_wait(1, part_r, k)
        means += part_r[lax.rem(y + k, NY)].astype(jnp.float32)
    zp_s[...] = means.astype(jnp.bfloat16)
    zp_copy.start()

    mask_row = jnp.broadcast_to(mask_ref[...].reshape(1, docs).astype(jnp.float32), (8, docs))
    lane2 = lax.broadcasted_iota(jnp.int32, (8, 256), 1)
    for j in range(NY):
        moved = mask_row if j == 0 else pltpu.roll(mask_row, docs - j * share, 1)
        mask4[j] = jnp.where(lane2 < share, moved[:, 0:256], 0.0)
    row2 = lax.broadcasted_iota(jnp.int32, (8, 256), 0)
    cutoff = jnp.zeros((8, 256), jnp.float32)
    mean_cutoff = jnp.float32(0.0)
    for m in range(members):
        cut = thr_ref[m].astype(jnp.float32) * (1.0 / 256.0)
        cutoff = jnp.where(row2 == m, cut, cutoff)
        mean_cutoff += cut * (1.0 / members)
    zc_copy.wait_recv()
    scores = zc_s[...] + zc_r[...]
    kept = mask4[y] * jax.nn.sigmoid(4.0 * (scores - cutoff))
    ens_score = jnp.sum(scores, axis=0, keepdims=True) * (1.0 / members)
    ens_kept = jax.nn.sigmoid(4.0 * (ens_score - mean_cutoff))
    kept_sum = jnp.sum(kept, axis=1, keepdims=True)
    agree_sum = jnp.sum(kept * ens_kept, axis=1, keepdims=True)
    lane = lax.broadcasted_iota(jnp.int32, (8, 128), 1)
    row = lax.broadcasted_iota(jnp.int32, (8, 128), 0)
    line = jnp.sum(
        jnp.where(lane == row, kept_sum, 0.0) + jnp.where(lane == row + 8, agree_sum, 0.0), axis=0, keepdims=True
    )
    first = y * NC + core
    tot1[first, 0:1, :] = line

    def tot1_copy(k):
        to = lax.rem(first + k, NY * NC)
        return pltpu.make_async_remote_copy(
            src_ref=tot1.at[first, pl.ds(0, 1)], dst_ref=tot1.at[first, pl.ds(0, 1)],
            send_sem=t_send.at[0], recv_sem=t_recv.at[0],
            device_id={"dp": dp_of(z, x, lax.rem(to, NC)), "ens": (to // NC) * NH + zh}, device_id_type=MESH,
        )

    for k in range(1, NY * NC):
        tot1_copy(k).start()
    peers = NY * NC - 1
    all1 = rcopy(tot1.at[pl.ds(0, peers), pl.ds(0, 1)], t_send.at[0], t_recv.at[0], sib)
    all1.wait_recv()
    line = tot1[0, 0:1, :]
    for k in range(1, NY * NC):
        line += tot1[k, 0:1, :]
    second = x * NZ + z
    tot2[second, 0:1, :] = line
    deep = zh * NZ + z
    for dx in range(NX):
        for dz in range(-NZ // 2, NZ // 2):
            if dx == 0 and dz == 0:
                continue
            zz = lax.rem(deep + dz + NZ * NH, NZ * NH)
            pltpu.make_async_remote_copy(
                src_ref=tot2.at[second, pl.ds(0, 1)], dst_ref=tot2.at[second, pl.ds(0, 1)],
                send_sem=t_send.at[1], recv_sem=t_recv.at[1],
                device_id={"dp": dp_of(lax.rem(zz, NZ), lax.rem(x + dx, NX), core), "ens": y * NH + zz // NZ},
                device_id_type=MESH,
            ).start()

    zp_copy.wait_recv()
    fin[y] = (zp_s[...].astype(jnp.float32) + zp_r[...].astype(jnp.float32)).astype(jnp.bfloat16)
    for k in range(1, NY):
        fin_copy(k).start()

    column = w.at[:, :, 0]
    rcopy(column, x_send.at[0], d_recv.at[0], sib).wait_send()
    rcopy(column, x_send.at[1], d_recv.at[0], sib).wait_send()
    rcopy(column, x_send.at[2], d_recv.at[0], sib).wait_send()
    rcopy(w.at[:, :, pl.ds(0, NX)], d_send.at[0], d_recv.at[0], sib).wait_send()
    block = w.at[:, 0, 0]
    for s in range(NZ - 1):
        @pl.when(has_zu & (z - s >= 0))
        def _():
            rcopy(block, z_send.at[0, s], d_recv.at[0], sib).wait_send()

        @pl.when(has_zd & (z + s < NZ))
        def _():
            rcopy(block, z_send.at[1, s], d_recv.at[0], sib).wait_send()
    for k in range(1, NY):
        sc_copy(k).wait_send()
        part_copy(k).wait_send()
    zc_copy.wait_send()
    zp_copy.wait_send()
    all1.wait_send()

    out_ref[pl.ds(pl.multiple_of(y * share, share), share), :] = fin[y].astype(jnp.float32)
    for k in range(1, NY):
        y_wait(2, fin, k)
        other = lax.rem(y + k, NY)
        out_ref[pl.ds(pl.multiple_of(other * share, share), share), :] = fin[other].astype(jnp.float32)
    for k in range(1, NY):
        fin_copy(k).wait_send()

    all2 = rcopy(tot2.at[pl.ds(0, NX * NZ - 1), pl.ds(0, 1)], t_send.at[1], t_recv.at[1], sib)
    all2.wait_recv()
    line = tot2[0, 0:1, :]
    for k in range(1, NX * NZ):
        line += tot2[k, 0:1, :]
    line = line * (1.0 / docs)
    at = lax.broadcasted_iota(jnp.int32, (1, 128), 1)
    kept_ref[0] = jnp.sum(jnp.where(at == ens, line, 0.0))
    agree_ref[0] = jnp.sum(jnp.where(at == ens + 8, line, 0.0))
    all2.wait_send()


def solution(mesh):
    def on_device(embeddings, valid_mask, first_weight, second_weight, thresholds):
        docs, width = embeddings.shape
        members, rows, units = first_weight.shape
        classes = second_weight.shape[2]
        share = docs // NY
        dma = pltpu.SemaphoreType.DMA
        bf16, f32 = jnp.bfloat16, jnp.float32
        hbm, vmem, smem = (pl.BlockSpec(memory_space=s) for s in (pl.ANY, pltpu.VMEM, pltpu.SMEM))
        return pl.pallas_call(
            kernel,
            out_shape=(
                jax.ShapeDtypeStruct((docs, classes), f32),
                jax.ShapeDtypeStruct((1,), f32),
                jax.ShapeDtypeStruct((1,), f32),
            ),
            in_specs=[hbm, vmem, hbm, hbm, smem],
            out_specs=(vmem, smem, smem),
            scratch_shapes=[
                pltpu.VMEM((members, NZ, NX * NC, rows, units), bf16),
                pltpu.VMEM((docs, width), bf16),
                pltpu.VMEM((members, units, 2 * classes), bf16),
                pltpu.VMEM((docs, 2 * classes), f32),
                pltpu.VMEM((NY, share, classes), bf16),
                pltpu.VMEM((NY, share, classes), bf16),
                pltpu.VMEM((NY, 8, 256), f32),
                pltpu.VMEM((NY, 8, 256), f32),
                pltpu.VMEM((share, classes), bf16),
                pltpu.VMEM((share, classes), bf16),
                pltpu.VMEM((8, 256), f32),
                pltpu.VMEM((8, 256), f32),
                pltpu.VMEM((NY, share, classes), bf16),
                pltpu.VMEM((NY, 8, 256), f32),
                pltpu.VMEM((NY * NC, 8, 128), f32),
                pltpu.VMEM((NX * NZ, 8, 128), f32),
                dma((3,)),
                dma((CHUNKS, NZ)),
                dma((CHUNKS, NZ, 3)),
                dma((CHUNKS,)),
                dma((2, NZ)),
                dma((3,)),
                dma((1,)),
                dma((3, NY)),
                dma((3, NY)),
                dma((2,)),
                dma((2,)),
                dma((2,)),
                dma((2,)),
            ],
            compiler_params=pltpu.CompilerParams(
                collective_id=0, has_side_effects=True, vmem_limit_bytes=63 * 1024 * 1024
            ),
        )(embeddings, valid_mask, first_weight, second_weight, thresholds)

    return jax.shard_map(
        on_device,
        mesh=mesh,
        in_specs=(P("dp", None), P("dp"), P(None, "dp", "ens"), P(None, "ens", None), P()),
        out_specs=(P("dp", None), P("ens"), P("ens")),
        check_vma=False,
    )
```
